32 devices in a mesh: dp: 4 (over y, x), centers: 8 (over z, core).
Axes of the slice: x: 2, y: 2, z: 4, core: 2. Of those that a mesh axis runs over, the one named last changes fastest.
Arguments:
- points: bfloat16 [16384, 32], P('dp'), may hold values from -6 to 6
- centers: bfloat16 [16384, 32], P('centers'), may hold values from -6 to 6
- coef: bfloat16 [16384, 64], P('centers'), may hold values from -0.1875 to 0.1875
Outputs:
- product: float32 [16384, 64], P('centers')
The draws below stay inside these ranges and needn't reach their ends.
All inputs are finite; a program needn't handle non-finite values.
Results may differ from the reference program's by a relative error of at most 0.0003.
Values may be sent and summed in bfloat16 or wider, within the bound.
No kernel may reach another device: no remote copies, remote signals or barrier semaphores. Data moves between devices by JAX's collectives and lax.ppermute only.
A program may use at most 128 MiB of HBM per device.

```python
import jax
import jax.numpy as jnp
from jax import lax

DIM = 32
OUTS = 64
NPTS = 16384
CENTERS = 16384


def block_scale(key, shape, shards, low, top_value):
    gain, own = 1.0, jax.random.fold_in(key, 6)
    for axis_at, blocks in shards:
        heights = jnp.exp(jax.random.uniform(jax.random.fold_in(own, axis_at), (blocks,), jnp.float32, low / len(shards), top_value / len(shards)))
        gain = gain * jnp.repeat(heights, shape[axis_at] // blocks).reshape([-1 if axis == axis_at else 1 for axis in range(len(shape))])
    return gain


def scatter_about(rng, shape, scale, limit, cuts=(), kind=jnp.bfloat16):
    values = jax.random.normal(rng, shape, jnp.float32) * scale
    if len(cuts) > 0:
        values = block_scale(rng, shape, cuts, -0.22, 0.18) * values
    return jnp.clip(values, min=-limit, max=limit).astype(kind)


def setup_inputs(seed: int = 0) -> dict:
    key_list = jax.random.split(jax.random.key(seed), 4)
    return {
        "points": scatter_about(key_list[0], (NPTS, DIM), 1.0, 6.0, ((0, 4),)),
        "centers": scatter_about(key_list[1], (CENTERS, DIM), 1.0, 6.0, ((0, 8),)),
        "coef": scatter_about(key_list[2], (CENTERS, OUTS), (CENTERS // 16) ** -0.5, 0.1875, ((0, 8),)),
    }


def kernel_block(left_pts, left_sq, right_pts, right_sq, features):
    inner = lax.dot_general(left_pts, right_pts, (((1,), (1,)), ((), ())), preferred_element_type=jnp.float32)
    dist = left_sq[:, None] + right_sq[None, :] - 2.0 * inner
    return jnp.exp(dist * (-2.0 / features)).astype(jnp.bfloat16)

def squares(values):
    wide = values.astype(jnp.float32)
    return lax.optimization_barrier(jnp.sum(wide * wide, axis=1))

def reference(points, centers, coef):
    features = points.shape[1]
    total_pts = points.shape[0]
    total_cen = centers.shape[0]
    outs_count = coef.shape[1]
    block_pts = min(1024, total_pts)
    cen_sq = squares(centers)
    point_blocks = points.reshape(total_pts // block_pts, block_pts, features)

    def data_step(accum, block):
        kernel = kernel_block(block, squares(block), centers, cen_sq, features)
        forward = jnp.dot(kernel, coef, preferred_element_type=jnp.float32).astype(jnp.bfloat16)
        back = lax.dot_general(kernel, forward, (((0,), (0,)), ((), ())), preferred_element_type=jnp.float32)
        return (accum + back, jnp.zeros((), jnp.float32))
    accum, unused = lax.scan(data_step, jnp.zeros((total_cen, outs_count), jnp.float32), point_blocks)
    block_cen = min(1024, total_cen)
    center_blocks = centers.reshape(total_cen // block_cen, block_cen, features)

    def center_step(carry, block):
        kernel = kernel_block(block, squares(block), centers, cen_sq, features)
        return (carry, jnp.dot(kernel, coef, preferred_element_type=jnp.float32))
    unused_two, regular = lax.scan(center_step, jnp.zeros((), jnp.float32), center_blocks)
    regular = regular.reshape(total_cen, outs_count)
    return accum * (1.0 / jnp.sqrt(jnp.float32(total_pts))) + regular
```

```python
import math

import jax
import jax.numpy as jnp
from jax import lax
from jax.experimental import pallas as pl
from jax.experimental.pallas import tpu as pltpu
from jax.sharding import PartitionSpec as P


TILE = 16
ROW_BLOCK = 512
COL_BLOCK = 512


def prepare(feats, values):
    count = len(feats)

    def body(*refs):
        for at in range(count):
            feat_ref, out_ref = refs[at], refs[count + len(present) + at]
            features, cols = feat_ref.shape
            wide = feat_ref[...].astype(jnp.float32)
            half = -0.5 * jnp.sum(wide * wide, axis=0, keepdims=True)
            high = half.astype(jnp.bfloat16).astype(jnp.float32)
            rest = half - high
            mid = rest.astype(jnp.bfloat16).astype(jnp.float32)
            low = rest - mid
            row = lax.broadcasted_iota(jnp.int32, (TILE, cols), 0)
            norm = jnp.where(row == 0, high, jnp.where(row == 1, mid, jnp.where(row == 2, low, 0.0)))
            out_ref[0:features, :] = feat_ref[...]
            out_ref[features : features + TILE, :] = norm.astype(jnp.bfloat16)
            if values[at] is not None:
                out_ref[features + TILE :, :] = refs[count + present.index(at)][...]

    present = [at for at in range(count) if values[at] is not None]
    shapes = [
        (feat.shape[0] + TILE + (0 if value is None else value.shape[0]), feat.shape[1])
        for feat, value in zip(feats, values)
    ]
    return pl.pallas_call(
        body,
        out_shape=[jax.ShapeDtypeStruct(shape, jnp.bfloat16) for shape in shapes],
    )(*feats, *[values[at] for at in present])


def product(rows, right, features, acc=None, base=None, start=None, span=None, norm=1.0, chunks=None, dtype=jnp.float32):
    AUG = features + TILE
    scale = math.log2(math.e) * 4.0 / features
    packed = not isinstance(rows, tuple)
    outs = rows.shape[0] - AUG if packed else rows[1].shape[1]
    low, cols = (0, right.shape[1]) if span is None else span
    shape = (outs, cols) if chunks is None else (chunks, outs, cols // chunks)
    pieces, piece = (1, rows.shape[1]) if packed else (rows[1].shape[0], rows[1].shape[2])
    row_block = min(ROW_BLOCK, piece)
    col_block = min(COL_BLOCK, cols)

    def body(*refs):
        refs = list(refs)
        base_ref = None if base is None else refs.pop(0)
        start_ref = None if start is None else refs.pop(0)
        left_ref = refs.pop(0)
        vals_ref = left_ref if packed else refs.pop(0)
        right_ref = refs.pop(0)
        first_ref = None if acc is None else refs.pop(0)
        out_ref, acc_ref = refs
        begin = 0 if base is None else pl.multiple_of(base_ref[0], piece)
        acc_ref[...] = jnp.zeros_like(acc_ref)

        ones = jnp.ones((TILE, max(row_block, col_block)), jnp.bfloat16)
        shift = low if start is None else pl.multiple_of(start_ref[0], cols)

        def inner(left, col):
            cut = pl.ds(shift + col, col_block)
            right = jnp.concatenate(
                [right_ref[0:features, cut], ones[:, :col_block], right_ref[features:AUG, cut]], axis=0
            )
            return jnp.dot(left, right, preferred_element_type=jnp.float32)

        def finish(state):
            vals, col, value = state
            kernel = jnp.exp2(value * scale).astype(jnp.bfloat16)
            acc_ref[:, col : col + col_block] += jnp.dot(vals, kernel, preferred_element_type=jnp.float32)

        state = None
        for at in range(pieces):
            for row in range(0, piece, row_block):
                left = left_ref[0:AUG, pl.ds(begin + at * piece + row, row_block)]
                left = jnp.concatenate([left, ones[:, :row_block]], axis=0).T
                if packed:
                    vals = vals_ref[AUG : AUG + outs, row : row + row_block]
                else:
                    vals = vals_ref[at, :, row : row + row_block]
                for col in range(0, cols, col_block):
                    value = inner(left, col)
                    if state is not None:
                        finish(state)
                    state = (vals, col, value)
        finish(state)

        width = cols if chunks is None else cols // chunks
        for at in range(cols // width):
            cut = slice(at * width, (at + 1) * width)
            total = acc_ref[:, cut]
            if norm != 1.0:
                total = total * norm
            if first_ref is not None:
                total = total + first_ref[:, low + at * width : low + (at + 1) * width]
            if chunks is None:
                out_ref[...] = total.astype(dtype)
            else:
                out_ref[at] = total.astype(dtype)

    vmem = pl.BlockSpec(memory_space=pltpu.VMEM)
    args = ([rows] if packed else list(rows)) + [right] + ([] if acc is None else [acc])
    specs = [vmem] * len(args)
    scalars = [value for value in (base, start) if value is not None]
    args = scalars + args
    specs = [pl.BlockSpec(memory_space=pltpu.SMEM)] * len(scalars) + specs
    count = pieces * piece
    return pl.pallas_call(
        body,
        in_specs=specs,
        out_specs=vmem,
        out_shape=jax.ShapeDtypeStruct(shape, dtype),
        scratch_shapes=[pltpu.VMEM((outs, cols), jnp.float32)],
        cost_estimate=pl.CostEstimate(
            flops=2 * count * cols * (AUG + outs), transcendentals=count * cols, bytes_accessed=2**21
        ),
    )(*args)


def source_group(dp_at, group_at, groups):
    if groups == 4:
        return ((0, 2, 1, 3), (1, 3, 0, 2), (2, 0, 3, 1), (3, 1, 2, 0))[dp_at][group_at]
    return (dp_at + group_at) % groups


def solution(mesh):
    dp_size = mesh.shape["dp"]
    cen_size = mesh.shape["centers"]
    pairs = cen_size // 2
    members = cen_size // dp_size
    swap = [(at, at ^ 1) for at in range(cen_size)]
    pair_groups = [[2 * at + core for at in range(pairs)] for core in range(2)]
    fetch = [
        (d * cen_size + source_group(d, g, dp_size) * members + m, d * cen_size + g * members + m)
        for d in range(dp_size)
        for g in range(dp_size)
        for m in range(members)
    ]

    def on_device(points, centers, coef):
        features = points.shape[1]
        local_pts = points.shape[0]
        half_pts = local_pts // 2
        total_pts = local_pts * dp_size
        core = lax.axis_index("centers") % 2
        own_base = (core * half_pts).astype(jnp.int32).reshape(1)

        pack, pts = prepare((centers.T, points.T), (coef.T, None))
        partner = lax.ppermute(pack, "centers", swap)
        fetched = lax.ppermute(pack, ("dp", "centers"), fetch)

        own_cols = dict(features=features, start=own_base, span=(0, half_pts))
        mine = product(pack, pts, **own_cols)
        partner, mine = lax.optimization_barrier((partner, mine))
        parts = product(partner, pts, acc=mine, chunks=pairs, dtype=jnp.bfloat16, **own_cols)
        others = [fetched]
        for step in range(1, members):
            ring = [
                (g * members + (m + step) % members, g * members + m)
                for g in range(dp_size)
                for m in range(members)
            ]
            others.append(lax.ppermute(fetched, "centers", ring))

        parts, others[0] = lax.optimization_barrier((parts, others[0]))
        regular = product(others[0], pack, features)
        parts = lax.all_to_all(parts, "centers", 0, 0, axis_index_groups=pair_groups)
        parts, regular = lax.optimization_barrier((parts, regular))
        shared = jnp.sum(parts.astype(jnp.float32), axis=0).astype(jnp.bfloat16)
        spread = jnp.broadcast_to(shared[None], (pairs,) + shared.shape)
        spread, regular = lax.optimization_barrier((spread, regular))
        first = lax.all_to_all(spread, "centers", 0, 0, axis_index_groups=pair_groups)
        for other in others[1:]:
            regular = product(other, pack, features, regular)
        first, regular = lax.optimization_barrier((first, regular))
        second = lax.ppermute(first, "centers", swap)

        norm = 1.0 / math.sqrt(total_pts)
        acc = product((pts, first), pack, features, regular, own_base, norm=norm)
        second, acc = lax.optimization_barrier((second, acc))
        half_cols = centers.shape[0] // 2
        rows = (pts, second)
        back_a = product(
            rows, pack, features, acc, half_pts - own_base, None, (0, half_cols), norm, dp_size
        )
        sums_a = scatter_sum(back_a)
        back_b = product(
            rows, pack, features, acc, half_pts - own_base, None, (half_cols, half_cols), norm, dp_size
        )
        sums_a, back_b = lax.optimization_barrier((sums_a, back_b))
        sum_a = sum(sums_a[1:], sums_a[0])
        sum_b = jnp.sum(lax.all_to_all(back_b, "dp", 0, 0), axis=0)
        both = jnp.stack([sum_a, sum_b])
        spread = jnp.broadcast_to(both[None], (dp_size,) + both.shape)
        whole = lax.all_to_all(spread, "dp", 0, 0)
        return whole.transpose(1, 0, 3, 2).reshape(centers.shape[0], coef.shape[1])

    def scatter_sum(parts):
        at = lax.axis_index("dp")
        pick = lambda step: lax.dynamic_index_in_dim(parts, (at + step) % dp_size, 0, keepdims=False)
        got = [pick(0)]
        for step in range(1, dp_size):
            ring = [(d, (d + step) % dp_size) for d in range(dp_size)]
            got.append(lax.ppermute(pick(step), "dp", ring))
        return got

    in_specs = (P("dp", None), P("centers", None), P("centers", None))

    return jax.shard_map(on_device, mesh=mesh, in_specs=in_specs, out_specs=P("centers", None), check_vma=False)
```

```python
import math

import jax
import jax.numpy as jnp
from jax import lax
from jax.experimental import pallas as pl
from jax.experimental.pallas import tpu as pltpu
from jax.sharding import PartitionSpec as P


TILE = 16
ROW_BLOCK = 512
COL_BLOCK = 512


def prepare(feats, values):
    count = len(feats)

    def body(*refs):
        for at in range(count):
            feat_ref, out_ref = refs[at], refs[count + len(present) + at]
            features, cols = feat_ref.shape
            wide = feat_ref[...].astype(jnp.float32)
            half = -0.5 * jnp.sum(wide * wide, axis=0, keepdims=True)
            high = half.astype(jnp.bfloat16).astype(jnp.float32)
            rest = half - high
            mid = rest.astype(jnp.bfloat16).astype(jnp.float32)
            low = rest - mid
            row = lax.broadcasted_iota(jnp.int32, (TILE, cols), 0)
            norm = jnp.where(row == 0, high, jnp.where(row == 1, mid, jnp.where(row == 2, low, 0.0)))
            out_ref[0:features, :] = feat_ref[...]
            out_ref[features : features + TILE, :] = norm.astype(jnp.bfloat16)
            if values[at] is not None:
                out_ref[features + TILE :, :] = refs[count + present.index(at)][...]

    present = [at for at in range(count) if values[at] is not None]
    shapes = [
        (feat.shape[0] + TILE + (0 if value is None else value.shape[0]), feat.shape[1])
        for feat, value in zip(feats, values)
    ]
    return pl.pallas_call(
        body,
        out_shape=[pltpu.VMEM(shape, jnp.bfloat16) for shape in shapes],
    )(*feats, *[values[at] for at in present])


def product(rows, right, features, acc=None, base=None, start=None, span=None, norm=1.0, chunks=None, dtype=jnp.float32):
    AUG = features + TILE
    scale = math.log2(math.e) * 4.0 / features
    packed = not isinstance(rows, tuple)
    outs = rows.shape[0] - AUG if packed else rows[1].shape[1]
    low, cols = (0, right.shape[1]) if span is None else span
    shape = (outs, cols) if chunks is None else (chunks, outs, cols // chunks)
    pieces, piece = (1, rows.shape[1]) if packed else (rows[1].shape[0], rows[1].shape[2])
    row_block = min(ROW_BLOCK, piece)
    col_block = min(COL_BLOCK, cols)

    def body(*refs):
        refs = list(refs)
        base_ref = None if base is None else refs.pop(0)
        start_ref = None if start is None else refs.pop(0)
        left_ref = refs.pop(0)
        vals_ref = left_ref if packed else refs.pop(0)
        right_ref = refs.pop(0)
        first_ref = None if acc is None else refs.pop(0)
        out_ref, acc_ref = refs
        begin = 0 if base is None else pl.multiple_of(base_ref[0], piece)
        acc_ref[...] = jnp.zeros_like(acc_ref)

        ones = jnp.ones((TILE, max(row_block, col_block)), jnp.bfloat16)
        shift = low if start is None else pl.multiple_of(start_ref[0], cols)

        def inner(left, col):
            cut = pl.ds(shift + col, col_block)
            right = jnp.concatenate(
                [right_ref[0:features, cut], ones[:, :col_block], right_ref[features:AUG, cut]], axis=0
            )
            return jnp.dot(left, right, preferred_element_type=jnp.float32)

        def finish(state):
            vals, col, value = state
            kernel = jnp.exp2(value * scale).astype(jnp.bfloat16)
            acc_ref[:, col : col + col_block] += jnp.dot(vals, kernel, preferred_element_type=jnp.float32)

        state = None
        for at in range(pieces):
            for row in range(0, piece, row_block):
                left = left_ref[0:AUG, pl.ds(begin + at * piece + row, row_block)]
                left = jnp.concatenate([left, ones[:, :row_block]], axis=0).T
                if packed:
                    vals = vals_ref[AUG : AUG + outs, row : row + row_block]
                else:
                    vals = vals_ref[at, :, row : row + row_block]
                for col in range(0, cols, col_block):
                    value = inner(left, col)
                    if state is not None:
                        finish(state)
                    state = (vals, col, value)
        finish(state)

        width = cols if chunks is None else cols // chunks
        for at in range(cols // width):
            cut = slice(at * width, (at + 1) * width)
            total = acc_ref[:, cut]
            if norm != 1.0:
                total = total * norm
            if first_ref is not None:
                total = total + first_ref[:, low + at * width : low + (at + 1) * width]
            if chunks is None:
                out_ref[...] = total.astype(dtype)
            else:
                out_ref[at] = total.astype(dtype)

    vmem = pl.BlockSpec(memory_space=pltpu.VMEM)
    args = ([rows] if packed else list(rows)) + [right] + ([] if acc is None else [acc])
    specs = [vmem] * len(args)
    args = [pltpu.with_memory_space_constraint(arg, pltpu.VMEM) for arg in args]
    scalars = [value for value in (base, start) if value is not None]
    args = scalars + args
    specs = [pl.BlockSpec(memory_space=pltpu.SMEM)] * len(scalars) + specs
    count = pieces * piece
    return pl.pallas_call(
        body,
        in_specs=specs,
        out_specs=vmem,
        out_shape=pltpu.VMEM(shape, dtype),
        scratch_shapes=[pltpu.VMEM((outs, cols), jnp.float32)],
        cost_estimate=pl.CostEstimate(
            flops=2 * count * cols * (AUG + outs), transcendentals=count * cols, bytes_accessed=2**21
        ),
    )(*args)


def source_group(dp_at, group_at, groups):
    if groups == 4:
        return ((0, 2, 1, 3), (1, 3, 0, 2), (2, 0, 3, 1), (3, 1, 2, 0))[dp_at][group_at]
    return (dp_at + group_at) % groups


def solution(mesh):
    dp_size = mesh.shape["dp"]
    cen_size = mesh.shape["centers"]
    pairs = cen_size // 2
    members = cen_size // dp_size
    swap = [(at, at ^ 1) for at in range(cen_size)]
    pair_groups = [[2 * at + core for at in range(pairs)] for core in range(2)]
    fetch = [
        (d * cen_size + source_group(d, g, dp_size) * members + m, d * cen_size + g * members + m)
        for d in range(dp_size)
        for g in range(dp_size)
        for m in range(members)
    ]

    def on_device(points, centers, coef):
        features = points.shape[1]
        local_pts = points.shape[0]
        half_pts = local_pts // 2
        total_pts = local_pts * dp_size
        core = lax.axis_index("centers") % 2
        own_base = (core * half_pts).astype(jnp.int32).reshape(1)

        pack, pts = prepare((centers.T, points.T), (coef.T, None))
        partner = lax.ppermute(pack, "centers", swap)
        fetched = lax.ppermute(pack, ("dp", "centers"), fetch)

        own_cols = dict(features=features, start=own_base, span=(0, half_pts))
        mine = product(pack, pts, **own_cols)
        partner, mine = lax.optimization_barrier((partner, mine))
        parts = product(partner, pts, acc=mine, chunks=pairs, dtype=jnp.bfloat16, **own_cols)
        others = [fetched]
        for step in range(1, members):
            ring = [
                (g * members + (m + step) % members, g * members + m)
                for g in range(dp_size)
                for m in range(members)
            ]
            others.append(lax.ppermute(fetched, "centers", ring))

        parts, others[0] = lax.optimization_barrier((parts, others[0]))
        regular = product(others[0], pack, features)
        parts = lax.all_to_all(parts, "centers", 0, 0, axis_index_groups=pair_groups)
        parts, regular = lax.optimization_barrier((parts, regular))
        shared = jnp.sum(parts.astype(jnp.float32), axis=0).astype(jnp.bfloat16)
        spread = jnp.broadcast_to(shared[None], (pairs,) + shared.shape)
        spread, regular = lax.optimization_barrier((spread, regular))
        first = lax.all_to_all(spread, "centers", 0, 0, axis_index_groups=pair_groups)
        for other in others[1:]:
            regular = product(other, pack, features, regular)
        first, regular = lax.optimization_barrier((first, regular))
        second = lax.ppermute(first, "centers", swap)

        norm = 1.0 / math.sqrt(total_pts)
        acc = product((pts, first), pack, features, regular, own_base, norm=norm)
        second, acc = lax.optimization_barrier((second, acc))
        half_cols = centers.shape[0] // 2
        rows = (pts, second)
        back_a = product(
            rows, pack, features, acc, half_pts - own_base, None, (0, half_cols), norm, dp_size
        )
        sums_a = scatter_sum(back_a)
        back_b = product(
            rows, pack, features, acc, half_pts - own_base, None, (half_cols, half_cols), norm, dp_size
        )
        sums_a, back_b = lax.optimization_barrier((sums_a, back_b))
        sum_a = sum(sums_a[1:], sums_a[0])
        sum_b = jnp.sum(lax.all_to_all(back_b, "dp", 0, 0), axis=0)
        both = jnp.stack([sum_a, sum_b])
        spread = jnp.broadcast_to(both[None], (dp_size,) + both.shape)
        whole = lax.all_to_all(spread, "dp", 0, 0)
        return whole.transpose(1, 0, 3, 2).reshape(centers.shape[0], coef.shape[1])

    def scatter_sum(parts):
        at = lax.axis_index("dp")
        pick = lambda step: lax.dynamic_index_in_dim(parts, (at + step) % dp_size, 0, keepdims=False)
        got = [pick(0)]
        for step in range(1, dp_size):
            ring = [(d, (d + step) % dp_size) for d in range(dp_size)]
            got.append(lax.ppermute(pick(step), "dp", ring))
        return got

    in_specs = (P("dp", None), P("centers", None), P("centers", None))

    return jax.shard_map(on_device, mesh=mesh, in_specs=in_specs, out_specs=P("centers", None), check_vma=False)
```

```python
import math

import jax
import jax.numpy as jnp
from jax import lax
from jax.experimental import pallas as pl
from jax.experimental.pallas import tpu as pltpu
from jax.sharding import PartitionSpec as P


TILE = 16
ROW_BLOCK = 512
COL_BLOCK = 512


def prepare(feats, values):
    count = len(feats)

    def body(*refs):
        for at in range(count):
            feat_ref, out_ref = refs[at], refs[count + len(present) + at]
            features, cols = feat_ref.shape
            wide = feat_ref[...].astype(jnp.float32)
            half = -0.5 * jnp.sum(wide * wide, axis=0, keepdims=True)
            high = half.astype(jnp.bfloat16).astype(jnp.float32)
            rest = half - high
            mid = rest.astype(jnp.bfloat16).astype(jnp.float32)
            low = rest - mid
            row = lax.broadcasted_iota(jnp.int32, (TILE, cols), 0)
            norm = jnp.where(row == 0, high, jnp.where(row == 1, mid, jnp.where(row == 2, low, 0.0)))
            out_ref[0:features, :] = feat_ref[...]
            out_ref[features : features + TILE, :] = norm.astype(jnp.bfloat16)
            if values[at] is not None:
                out_ref[features + TILE :, :] = refs[count + present.index(at)][...]

    present = [at for at in range(count) if values[at] is not None]
    shapes = [
        (feat.shape[0] + TILE + (0 if value is None else value.shape[0]), feat.shape[1])
        for feat, value in zip(feats, values)
    ]
    return pl.pallas_call(
        body,
        out_shape=[pltpu.VMEM(shape, jnp.bfloat16) for shape in shapes],
    )(*feats, *[values[at] for at in present])


def product(rows, right, features, acc=None, base=None, start=None, span=None, norm=1.0, chunks=None, dtype=jnp.float32):
    AUG = features + TILE
    scale = math.log2(math.e) * 4.0 / features
    packed = not isinstance(rows, tuple)
    outs = rows.shape[0] - AUG if packed else rows[1].shape[1]
    low, cols = (0, right.shape[1]) if span is None else span
    shape = (outs, cols) if chunks is None else (chunks, outs, cols // chunks)
    pieces, piece = (1, rows.shape[1]) if packed else (rows[1].shape[0], rows[1].shape[2])
    row_block = min(ROW_BLOCK, piece)
    col_block = min(COL_BLOCK, cols)

    def body(*refs):
        refs = list(refs)
        base_ref = None if base is None else refs.pop(0)
        start_ref = None if start is None else refs.pop(0)
        left_ref = refs.pop(0)
        vals_ref = left_ref if packed else refs.pop(0)
        right_ref = refs.pop(0)
        first_ref = None if acc is None else refs.pop(0)
        out_ref, acc_ref = refs
        begin = 0 if base is None else pl.multiple_of(base_ref[0], piece)
        acc_ref[...] = jnp.zeros_like(acc_ref)

        ones = jnp.ones((TILE, max(row_block, col_block)), jnp.bfloat16)
        shift = low if start is None else pl.multiple_of(start_ref[0], cols)

        def inner(left, col):
            cut = pl.ds(shift + col, col_block)
            right = jnp.concatenate(
                [right_ref[0:features, cut], ones[:, :col_block], right_ref[features:AUG, cut]], axis=0
            )
            return jnp.dot(left, right, preferred_element_type=jnp.float32)

        def finish(state):
            vals, col, value = state
            kernel = jnp.exp2(value * scale).astype(jnp.bfloat16)
            acc_ref[:, col : col + col_block] += jnp.dot(vals, kernel, preferred_element_type=jnp.float32)

        state = None
        for at in range(pieces):
            for row in range(0, piece, row_block):
                left = left_ref[0:AUG, pl.ds(begin + at * piece + row, row_block)]
                left = jnp.concatenate([left, ones[:, :row_block]], axis=0).T
                if packed:
                    vals = vals_ref[AUG : AUG + outs, row : row + row_block]
                else:
                    vals = vals_ref[at, :, row : row + row_block]
                for col in range(0, cols, col_block):
                    value = inner(left, col)
                    if state is not None:
                        finish(state)
                    state = (vals, col, value)
        finish(state)

        width = cols if chunks is None else cols // chunks
        for at in range(cols // width):
            cut = slice(at * width, (at + 1) * width)
            total = acc_ref[:, cut]
            if norm != 1.0:
                total = total * norm
            if first_ref is not None:
                total = total + first_ref[:, low + at * width : low + (at + 1) * width]
            if chunks is None:
                out_ref[...] = total.astype(dtype)
            else:
                out_ref[at] = total.astype(dtype)

    vmem = pl.BlockSpec(memory_space=pltpu.VMEM)
    args = ([rows] if packed else list(rows)) + [right] + ([] if acc is None else [acc])
    specs = [vmem] * len(args)
    args = [pltpu.with_memory_space_constraint(arg, pltpu.VMEM) for arg in args]
    scalars = [value for value in (base, start) if value is not None]
    args = scalars + args
    specs = [pl.BlockSpec(memory_space=pltpu.SMEM)] * len(scalars) + specs
    count = pieces * piece
    return pl.pallas_call(
        body,
        in_specs=specs,
        out_specs=vmem,
        out_shape=pltpu.VMEM(shape, dtype),
        scratch_shapes=[pltpu.VMEM((outs, cols), jnp.float32)],
        cost_estimate=pl.CostEstimate(
            flops=2 * count * cols * (AUG + outs), transcendentals=count * cols, bytes_accessed=2**21
        ),
    )(*args)


def source_group(dp_at, group_at, groups):
    if groups == 4:
        return ((0, 2, 1, 3), (1, 3, 0, 2), (2, 0, 3, 1), (3, 1, 2, 0))[dp_at][group_at]
    return (dp_at + group_at) % groups


def solution(mesh):
    dp_size = mesh.shape["dp"]
    cen_size = mesh.shape["centers"]
    pairs = cen_size // 2
    members = cen_size // dp_size
    swap = [(at, at ^ 1) for at in range(cen_size)]
    pair_groups = [[2 * at + core for at in range(pairs)] for core in range(2)]
    fetch = [
        (d * cen_size + source_group(d, g, dp_size) * members + m, d * cen_size + g * members + m)
        for d in range(dp_size)
        for g in range(dp_size)
        for m in range(members)
    ]

    def on_device(points, centers, coef):
        features = points.shape[1]
        local_pts = points.shape[0]
        half_pts = local_pts // 2
        total_pts = local_pts * dp_size
        core = lax.axis_index("centers") % 2
        own_base = (core * half_pts).astype(jnp.int32).reshape(1)

        pack, pts = prepare((centers.T, points.T), (coef.T, None))
        partner = lax.ppermute(pack, "centers", swap)
        fetched = lax.ppermute(pack, ("dp", "centers"), fetch)

        own_cols = dict(features=features, start=own_base, span=(0, half_pts))
        mine = product(pack, pts, **own_cols)
        partner, mine = lax.optimization_barrier((partner, mine))
        parts = product(partner, pts, acc=mine, chunks=pairs, dtype=jnp.bfloat16, **own_cols)
        others = [fetched]
        for step in range(1, members):
            ring = [
                (g * members + (m + step) % members, g * members + m)
                for g in range(dp_size)
                for m in range(members)
            ]
            others.append(lax.ppermute(fetched, "centers", ring))

        parts = lax.all_to_all(parts, "centers", 0, 0, axis_index_groups=pair_groups)
        regular = product(others[0], pack, features)
        parts, regular = lax.optimization_barrier((parts, regular))
        shared = jnp.sum(parts.astype(jnp.float32), axis=0).astype(jnp.bfloat16)
        spread = jnp.broadcast_to(shared[None], (pairs,) + shared.shape)
        spread, regular = lax.optimization_barrier((spread, regular))
        first = lax.all_to_all(spread, "centers", 0, 0, axis_index_groups=pair_groups)
        for other in others[1:]:
            regular = product(other, pack, features, regular)
        first, regular = lax.optimization_barrier((first, regular))
        second = lax.ppermute(first, "centers", swap)

        norm = 1.0 / math.sqrt(total_pts)
        acc = product((pts, first), pack, features, regular, own_base, norm=norm)
        second, acc = lax.optimization_barrier((second, acc))
        rows = (pts, second)
        back = product(rows, pack, features, acc, half_pts - own_base, norm=norm, chunks=dp_size)
        summed = jnp.sum(lax.all_to_all(back, "dp", 0, 0), axis=0)
        spread = jnp.broadcast_to(summed[None], (dp_size,) + summed.shape)
        whole = lax.all_to_all(spread, "dp", 0, 0)
        return whole.transpose(0, 2, 1).reshape(centers.shape[0], coef.shape[1])

    in_specs = (P("dp", None), P("centers", None), P("centers", None))

    return jax.shard_map(on_device, mesh=mesh, in_specs=in_specs, out_specs=P("centers", None), check_vma=False)
```
